32 devices in a mesh: rows: 8 (over z, x), grp: 4 (over y, core).
Axes of the slice: x: 2, y: 2, z: 4, core: 2. Of those that a mesh axis runs over, the one named last changes fastest.
Arguments:
- matrix: bfloat16 [10240, 16384], P(('rows', 'grp')), may hold values from -36 to 36
- sample_rows: int32 [32, 128, 256], P(('rows', 'grp')), may hold values from 0 to 319
- pair_list: int32 [8, 8, 4], replicated, may hold values from 0 to 255, as said below
- pair_count: int32 [8, 8], replicated, may hold values from 1 to 4, as said below
- pair_blocks: int32 [256, 2], replicated, may hold values from 0 to 127, as said below
Outputs:
- gram: float32 [256, 128, 128], P(('rows', 'grp'))
The draws below stay inside these ranges and needn't reach their ends.
Inputs may be any that keep to these rules, and one draw needn't show every extreme that they name: `pair_list`: entry [s, r, k] lies in [r * 32, (r + 1) * 32); the 4 entries of one [s, r] are distinct. `pair_count`: every row group has some owner with all 4 slots active, and some owner has all 4 slots active from every row group. `pair_blocks`: the two blocks of a pair differ.
All inputs are finite; a program needn't handle non-finite values.
Results may differ from the reference program's by a relative error of at most 0.0016.
Values sent between devices are 32-bit elements; how exact they have to be, the bound alone decides.
A program may use at most 192 MiB of HBM per device.

```python
import math
import jax
import jax.numpy as jnp
from jax import lax

BLOCK = 128
NB = 128
ROWS_DEV = 320
SAMP = 256
CAP = 4
NCOL = 16384
ROWS_TOTAL = 10240
PAIRS = 256
REGION = 32
N_ROWS = 8
N_GRP = 4
DEVICES = 32


def draw_matrix(key, part):
    key_base, key_row, key_col = jax.random.split(key, 3)
    row_scale = jnp.exp(jax.random.uniform(key_row, (ROWS_TOTAL, 1), jnp.float32, math.log(0.3), math.log(3.0)))
    col_scale = jnp.exp(jax.random.uniform(key_col, (1, NCOL), jnp.float32, math.log(0.5), math.log(2.0)))
    base = jnp.clip(jax.random.normal(key_base, (ROWS_TOTAL, NCOL), jnp.float32), -6.0, 6.0)
    return (base * row_scale * col_scale).astype(jnp.bfloat16)


def draw_pair_list(key, part):
    keys = jax.random.split(jax.random.fold_in(key, 11), N_ROWS * N_ROWS)
    chosen = jax.vmap(lambda single: jax.random.permutation(single, REGION)[:CAP])(keys)
    chosen = chosen.reshape(N_ROWS, N_ROWS, CAP).astype(jnp.int32)
    owner_base = (jnp.arange(N_ROWS, dtype=jnp.int32) * REGION)[None, :, None]
    return chosen + owner_base


def draw_pair_count(key, part):
    key_count, key_row, key_col = jax.random.split(jax.random.fold_in(key, 23), 3)
    counts = jax.random.randint(key_count, (N_ROWS, N_ROWS), 1, CAP + 1).astype(jnp.int32)
    full_owner = jax.random.randint(key_row, (N_ROWS,), 0, N_ROWS)
    counts = counts.at[jnp.arange(N_ROWS), full_owner].set(CAP)
    common_owner = jax.random.randint(key_col, (), 0, N_ROWS)
    counts = counts.at[:, common_owner].set(CAP)
    return counts.astype(jnp.int32)


def draw_pair_blocks(key, part):
    key_first, key_step = jax.random.split(jax.random.fold_in(key, 37))
    first_block = jax.random.randint(key_first, (PAIRS,), 0, NB)
    step_size = jax.random.randint(key_step, (PAIRS,), 1, NB)
    second_block = (first_block + step_size) % NB
    return jnp.stack([first_block, second_block], axis=1).astype(jnp.int32)


def touch_ends(result, rng, smallest, high):
    dims = result.shape
    place = [jax.random.randint(jax.random.fold_in(rng, axis), (), 0, dims[axis]) for axis in range(len(dims))]
    result = result.at[tuple(place)].set(smallest)
    longest = dims.index(max(dims))
    place[longest] = (place[longest] + 1) % dims[longest]
    return result.at[tuple(place)].set(high)


def setup_inputs(seed: int = 0) -> dict:
    seeds = jax.random.split(jax.random.key(seed), 6)
    return {
        "matrix": draw_matrix(jax.random.fold_in(seeds[5], 71), 0),
        "sample_rows": touch_ends(jax.random.randint(seeds[1], (DEVICES, NB, SAMP), 0, ROWS_DEV), jax.random.fold_in(seeds[1], 1), 0, ROWS_DEV - 1).astype(jnp.int32),
        "pair_list": draw_pair_list(jax.random.fold_in(seeds[5], 71), 0),
        "pair_count": draw_pair_count(jax.random.fold_in(seeds[5], 71), 0),
        "pair_blocks": draw_pair_blocks(jax.random.fold_in(seeds[5], 71), 0),
    }


def reference(matrix, sample_rows, pair_list, pair_count, pair_blocks):
    device_total = N_ROWS * N_GRP
    blocks_all = matrix.reshape(device_total, ROWS_DEV, NB, BLOCK)
    positions = jnp.arange(ROWS_DEV, dtype=jnp.int32)
    slot_numbers = jnp.arange(CAP, dtype=jnp.int32)

    def one_device(raw_tiles, device):
        source = device // N_GRP
        blocks = blocks_all[device]
        picked = sample_rows[device]
        multiplicity = lax.optimization_barrier(jnp.sum((picked[:, :, None] == positions[None, None, :]).astype(jnp.float32), axis=1))
        weighted = (jnp.transpose(multiplicity)[:, :, None] * blocks.astype(jnp.float32)).astype(jnp.bfloat16)
        pair_ids = pair_list[source].reshape(-1)
        live_mask = (slot_numbers[None, :] < pair_count[source][:, None]).reshape(-1).astype(jnp.float32)
        first_block = pair_blocks[pair_ids, 0]
        second_block = pair_blocks[pair_ids, 1]
        weighted_cols = jnp.take(weighted, first_block, axis=1).astype(jnp.float32)
        plain_cols = jnp.take(blocks, second_block, axis=1).astype(jnp.float32)
        partial_tiles = jnp.einsum('rgi,rgj->gij', weighted_cols, plain_cols)
        partial_tiles = partial_tiles * live_mask[:, None, None]
        return (raw_tiles.at[pair_ids].add(partial_tiles), None)
    start = jnp.zeros((PAIRS, BLOCK, BLOCK), jnp.float32)
    raw_tiles, _ = lax.scan(one_device, start, jnp.arange(device_total, dtype=jnp.int32))
    squares = lax.optimization_barrier(jnp.sum(jnp.square(matrix.astype(jnp.float32)), axis=0))
    root_mean = jnp.sqrt(squares / ROWS_TOTAL + 1e-06).reshape(NB, BLOCK)
    left_scale = root_mean[pair_blocks[:, 0]]
    right_scale = root_mean[pair_blocks[:, 1]]
    return raw_tiles / (SAMP * left_scale[:, :, None] * right_scale[:, None, :])
```

```python
import functools

import jax
import jax.numpy as jnp
from jax import lax
from jax.experimental import pallas as pl
from jax.experimental.pallas import tpu as pltpu
from jax.sharding import PartitionSpec as P

epsilon = 1e-06
MESH = pl.DeviceIdType.MESH
F32 = jnp.float32
BF16 = jnp.bfloat16


def kernel(
    dims, table, samples, matrix, out,
    mat, squares, sq_in, sq_half, sq_in2, sq_rows, sq_total,
    core_out, core_in, keep, row_in, part_a, part_b, part_c, part_d, in_a, in_b, in_c,
    load_sem, sq_send, sq_recv, sq_row_send, sq_row_recv,
    core_send, core_recv, row_send, row_recv,
    a_send, a_recv, b_send, b_recv, c_send, c_recv,
):
    row_count, grp_count, cap, pairs = dims
    block_count, rows_dev, width = mat.shape
    sample_count = samples.shape[1]
    half = cap // 2
    region = pairs // row_count
    tile_dev = region // grp_count
    count_at = row_count * row_count * cap
    first_at = count_at + row_count * row_count
    second_at = first_at + pairs

    s = lax.axis_index("rows")
    g = lax.axis_index("grp")
    low = lax.rem(g, 2)
    high = lax.div(g, 2)
    partner = high * 2 + (1 - low)
    across = (1 - high) * 2 + low

    def at(row, grp):
        return {"rows": row, "grp": grp}

    def send(source, target, send_sem, recv_sem, row, grp):
        return pltpu.make_async_remote_copy(
            src_ref=source, dst_ref=target, send_sem=send_sem, recv_sem=recv_sem,
            device_id=at(row, grp), device_id_type=MESH,
        )

    def load(i):
        source = matrix.at[:, pl.ds(pl.multiple_of(i * width, width), width)]
        return pltpu.make_async_copy(source, mat.at[i], load_sem.at[i])

    def load_go(i, carry):
        load(i).start()
        return carry

    lax.fori_loop(0, block_count, load_go, 0)

    barrier = pltpu.get_barrier_semaphore()
    pl.semaphore_signal(barrier, inc=1, device_id=at(s, partner), device_id_type=MESH)
    pl.semaphore_signal(barrier, inc=1, device_id=at(s, across), device_id_type=MESH)

    def greet(j, carry):
        row = lax.rem(s + j, row_count)
        pl.semaphore_signal(barrier, inc=1, device_id=at(row, g), device_id_type=MESH)
        return carry

    lax.fori_loop(1, row_count, greet, 0)

    zero_tile = jnp.zeros((width, width), F32)

    def clear(j, carry):
        row_in[j, half] = zero_tile
        return carry

    lax.fori_loop(0, row_count, clear, 0)

    def square_group(n, carry):
        lines = []
        for m in range(8):
            load(n * 8 + m).wait()
        for m in range(8):
            values = mat[n * 8 + m].astype(F32)
            lines.append(jnp.sum(values * values, axis=0, keepdims=True))
        squares[pl.ds(pl.multiple_of(n * 8, 8), 8), :] = jnp.concatenate(lines, axis=0)
        return carry

    lax.fori_loop(0, block_count // 8, square_group, 0)
    pl.semaphore_wait(barrier, row_count + 1)

    nb2 = block_count // 2
    nb4 = block_count // 4

    def span(start, size):
        return pl.ds(pl.multiple_of(start, 8), size)

    sq1 = send(squares.at[span((1 - low) * nb2, nb2)], sq_in, sq_send.at[0], sq_recv.at[0], s, partner)
    sq2 = send(sq_half.at[span((1 - high) * nb4, nb4)], sq_in2, sq_send.at[1], sq_recv.at[1], s, across)
    quarter = span(low * nb2 + high * nb4, nb4)
    sq4 = send(sq_total.at[quarter], sq_total.at[quarter], sq_send.at[2], sq_recv.at[2], s, across)
    my_half = span(low * nb2, nb2)
    sq5 = send(sq_total.at[my_half], sq_total.at[my_half], sq_send.at[3], sq_recv.at[3], s, partner)

    def sq_row(j):
        row = lax.rem(s + j, row_count)
        return send(sq_rows.at[s], sq_rows.at[s], sq_row_send.at[j], sq_row_recv.at[s], row, g)

    def sq_row_from(j):
        source = lax.rem(s + j, row_count)
        return send(sq_rows.at[source], sq_rows.at[source], sq_row_send.at[j], sq_row_recv.at[source], source, g)

    positions = lax.broadcasted_iota(jnp.int32, (rows_dev, sample_count), 0)
    ones = jnp.ones((sample_count, width), BF16)

    def slot_tile(owner, slot):
        pair = table[(s * row_count + owner) * cap + slot]
        active = (slot < table[count_at + s * row_count + owner]).astype(F32)
        first = table[first_at + pair]
        second = table[second_at + pair]
        picked = samples[first].reshape(1, sample_count)
        hits = jnp.where(positions == picked, 1.0, 0.0).astype(BF16)
        multiplicity = jnp.dot(hits, ones, preferred_element_type=F32)
        left = mat[first].astype(F32)
        right = mat[second]
        weighted = (multiplicity * active * left).astype(BF16)
        return lax.dot_general(
            weighted, right, (((0,), (0,)), ((), ())), preferred_element_type=F32
        )

    def core_copy(j):
        return send(core_out.at[j], core_in.at[j], core_send.at[j], core_recv.at[j], s, partner)

    def row_copy(j):
        owner = lax.rem(s + j, row_count)
        target = row_in.at[s, pl.ds(0, half)]
        return send(keep.at[j], target, row_send.at[j], row_recv.at[s], owner, g)

    def row_from(j):
        source = lax.rem(s + j, row_count)
        target = row_in.at[source, pl.ds(0, half)]
        return send(keep.at[j], target, row_send.at[j], row_recv.at[source], source, g)

    def make(j):
        owner = lax.rem(s + j, row_count)
        for n in range(half):
            core_out[j, n] = slot_tile(owner, (1 - low) * half + n)
        core_copy(j).start()
        for n in range(half):
            keep[j, n] = slot_tile(owner, low * half + n)

    def forward(j):
        core_copy(j).wait_recv()
        keep[j] = keep[j] + core_in[j]
        row_copy(j).start()

    def step(j, carry):
        make(j)
        forward(j - 1)
        return carry

    cut1 = min(3, row_count)
    cut2 = min(5, row_count)
    sq1.start()
    make(1)
    lax.fori_loop(2, cut1, step, 0)
    sq1.wait()
    sq_half[...] = squares[my_half, :] + sq_in[...]
    sq2.start()
    lax.fori_loop(cut1, cut2, step, 0)
    sq2.wait()
    sq_rows[s] = sq_half[span(high * nb4, nb4), :] + sq_in2[...]

    def sq_go(j, carry):
        sq_row(j).start()
        return carry

    lax.fori_loop(1, row_count, sq_go, 0)
    lax.fori_loop(cut2, row_count, step, 0)
    make(0)
    forward(row_count - 1)
    core_copy(0).wait_recv()
    row_in[s, pl.ds(0, half)] = keep[0] + core_in[0]

    def sq_done(j, carry):
        sq_row_from(j).wait_recv()
        return carry

    lax.fori_loop(1, row_count, sq_done, 0)
    sq_sum = sq_rows[0]
    for j in range(1, row_count):
        sq_sum = sq_sum + sq_rows[j]
    sq_total[quarter, :] = sq_sum
    sq4.start()

    def row_done(j, carry):
        row_from(j).wait_recv()
        return carry

    lax.fori_loop(1, row_count, row_done, 0)

    def owned(grp, n):
        pair = s * region + grp * tile_dev + n
        total = None
        for source in range(row_count):
            base = (source * row_count + s) * cap + low * half
            index = half
            for m in range(half):
                same = (table[base + m] == pair).astype(jnp.int32)
                index = jnp.minimum(index, half - (half - m) * same)
            tile = row_in[source, index]
            total = tile if total is None else total + tile
        return total

    def a_copy(n):
        return send(part_a.at[n], in_a.at[n], a_send.at[n], a_recv.at[n], s, partner)

    def b_copy(n):
        return send(part_b.at[n], in_b.at[n], b_send.at[n], b_recv.at[n], s, across)

    c_copy = send(part_c, in_c, c_send, c_recv, s, partner)
    far_low = (1 - high) * 2 + low
    far_other = (1 - high) * 2 + (1 - low)

    def pass_on(n):
        a_copy(n).wait_recv()
        part_b[n] = part_b[n] + in_a[n]
        b_copy(n).start()

    def far(n, carry):
        part_a[n] = owned(far_other, n)
        a_copy(n).start()
        part_b[n] = owned(far_low, n)

        @pl.when(n > 0)
        def _():
            pass_on(n - 1)

        return carry

    lax.fori_loop(0, tile_dev, far, 0)
    pass_on(tile_dev - 1)
    sq4.wait()
    sq5.start()

    def near_other(n, carry):
        part_c[n] = owned(partner, n)
        return carry

    lax.fori_loop(0, tile_dev, near_other, 0)
    c_copy.start()

    def near(n, carry):
        part_d[n] = owned(g, n)
        return carry

    lax.fori_loop(0, tile_dev, near, 0)
    sq5.wait()
    c_copy.wait()
    sq_total[...] = jnp.sqrt(
        sq_total[...] / (rows_dev * row_count * grp_count) + epsilon
    )

    def finish(n, carry):
        pair = s * region + g * tile_dev + n
        first = table[first_at + pair]
        second = table[second_at + pair]
        left = jnp.broadcast_to(sq_total[first].reshape(1, width), (width, width)).T
        right = sq_total[second].reshape(1, width)
        b_copy(n).wait_recv()
        total = part_d[n] + in_c[n] + in_b[n]
        out[n] = total / (sample_count * left * right)
        return carry

    lax.fori_loop(0, tile_dev, finish, 0)

    def drain_tiles(n, carry):
        a_copy(n).wait_send()
        b_copy(n).wait_send()
        return carry

    lax.fori_loop(0, tile_dev, drain_tiles, 0)

    def drain_rows(j, carry):
        core_copy(j).wait_send()
        row_copy(j).wait_send()
        sq_row(j).wait_send()
        return carry

    lax.fori_loop(1, row_count, drain_rows, 0)
    core_copy(0).wait_send()


def shards(matrix, sample_rows, pair_list, pair_count, pair_blocks):
    rows_dev, column_count = matrix.shape
    block_count, sample_count = sample_rows.shape[1:]
    width = column_count // block_count
    row_count = lax.axis_size("rows")
    grp_count = lax.axis_size("grp")
    cap = pair_list.shape[2]
    pairs = pair_blocks.shape[0]
    tile_dev = pairs // (row_count * grp_count)
    half = cap // 2
    table = jnp.concatenate(
        [
            pair_list.reshape(-1),
            pair_count.reshape(-1),
            pair_blocks[:, 0],
            pair_blocks[:, 1],
        ]
    )
    dma = pltpu.SemaphoreType.DMA

    def vmem(*shape):
        return pltpu.VMEM(shape, F32)

    some = vmem(tile_dev, width, width)
    nb2, nb4 = block_count // 2, block_count // 4
    return pl.pallas_call(
        functools.partial(kernel, (row_count, grp_count, cap, pairs)),
        out_shape=jax.ShapeDtypeStruct((tile_dev, width, width), F32),
        in_specs=[
            pl.BlockSpec(memory_space=pltpu.SMEM),
            pl.BlockSpec(memory_space=pltpu.VMEM),
            pl.BlockSpec(memory_space=pl.ANY),
        ],
        out_specs=pl.BlockSpec(memory_space=pltpu.VMEM),
        scratch_shapes=[
            pltpu.VMEM((block_count, rows_dev, width), BF16),
            vmem(block_count, width),
            vmem(nb2, width),
            vmem(nb2, width),
            vmem(nb4, width),
            vmem(row_count, nb4, width),
            vmem(block_count, width),
            vmem(row_count, half, width, width),
            vmem(row_count, half, width, width),
            vmem(row_count, half, width, width),
            vmem(row_count, half + 1, width, width),
            some, some, some, some, some, some, some,
            dma((block_count,)), dma((4,)), dma((4,)), dma((row_count,)), dma((row_count,)),
            dma((row_count,)), dma((row_count,)), dma((row_count,)), dma((row_count,)),
            dma((tile_dev,)), dma((tile_dev,)), dma((tile_dev,)), dma((tile_dev,)),
            dma, dma,
        ],
        compiler_params=pltpu.CompilerParams(
            collective_id=0, has_side_effects=True, vmem_limit_bytes=67043328
        ),
        name="gram_tiles",
    )(table, sample_rows[0], matrix)


def solution(mesh):
    in_specs = (P(("rows", "grp"), None), P(("rows", "grp"), None, None), P(), P(), P())
    out_specs = P(("rows", "grp"), None, None)
    return jax.shard_map(shards, mesh=mesh, in_specs=in_specs, out_specs=out_specs, check_vma=False)
```

```python
import functools

import jax
import jax.numpy as jnp
from jax import lax
from jax.experimental import pallas as pl
from jax.experimental.pallas import tpu as pltpu
from jax.sharding import PartitionSpec as P

epsilon = 1e-06
MESH = pl.DeviceIdType.MESH
F32 = jnp.float32
BF16 = jnp.bfloat16


def kernel(
    dims, pair_list, pair_count, pair_blocks, samples_hbm, matrix, out,
    mat, samples, sample_sem, squares, sq_in, sq_half, sq_in2, sq_rows, sq_total,
    core_out, core_in, keep, high_in, row_in, part_a, part_b, part_c, part_d, in_a, in_b, in_c,
    load_sem, sq_send, sq_recv, sq_row_send, sq_row_recv,
    core_send, core_recv, high_send, high_recv, row_send, row_recv,
    a_send, a_recv, b_send, b_recv, c_send, c_recv,
):
    row_count, grp_count, cap, pairs = dims
    block_count, rows_dev, width = mat.shape
    sample_count = samples.shape[1]
    half = cap // 2
    region = pairs // row_count
    tile_dev = region // grp_count
    quota = half // 2
    row_half = row_count // 2

    s = lax.axis_index("rows")
    g = lax.axis_index("grp")
    low = lax.rem(g, 2)
    high = lax.div(g, 2)
    partner = high * 2 + (1 - low)
    across = (1 - high) * 2 + low

    def at(row, grp):
        return {"rows": row, "grp": grp}

    def send(source, target, send_sem, recv_sem, row, grp):
        return pltpu.make_async_remote_copy(
            src_ref=source, dst_ref=target, send_sem=send_sem, recv_sem=recv_sem,
            device_id=at(row, grp), device_id_type=MESH,
        )

    def load(i):
        source = matrix.at[:, pl.ds(pl.multiple_of(i * width, width), width)]
        return pltpu.make_async_copy(source, mat.at[i], load_sem.at[i])

    def load_go(i, carry):
        load(i).start()
        return carry

    sample_load = pltpu.make_async_copy(samples_hbm, samples, sample_sem)
    sample_load.start()
    lax.fori_loop(0, block_count, load_go, 0)

    barrier = pltpu.get_barrier_semaphore()
    pl.semaphore_signal(barrier, inc=1, device_id=at(s, partner), device_id_type=MESH)
    pl.semaphore_signal(barrier, inc=1, device_id=at(s, across), device_id_type=MESH)

    def greet(j, carry):
        row = lax.rem(s + j, row_count)
        pl.semaphore_signal(barrier, inc=1, device_id=at(row, g), device_id_type=MESH)
        return carry

    lax.fori_loop(1, row_count, greet, 0)

    zero_tile = jnp.zeros((width, width), F32)

    def clear(j, carry):
        row_in[j, half] = zero_tile
        return carry

    lax.fori_loop(0, row_count, clear, 0)

    def square_group(n, carry):
        lines = []
        for m in range(8):
            load(n * 8 + m).wait()
        for m in range(8):
            values = mat[n * 8 + m].astype(F32)
            lines.append(jnp.sum(values * values, axis=0, keepdims=True))
        squares[pl.ds(pl.multiple_of(n * 8, 8), 8), :] = jnp.concatenate(lines, axis=0)
        return carry

    lax.fori_loop(0, block_count // 8, square_group, 0)
    sample_load.wait()
    pl.semaphore_wait(barrier, row_count + 1)

    nb2 = block_count // 2
    nb4 = block_count // 4

    def span(start, size):
        return pl.ds(pl.multiple_of(start, 8), size)

    sq1 = send(squares.at[span((1 - low) * nb2, nb2)], sq_in, sq_send.at[0], sq_recv.at[0], s, partner)
    sq2 = send(sq_half.at[span((1 - high) * nb4, nb4)], sq_in2, sq_send.at[1], sq_recv.at[1], s, across)
    quarter = span(low * nb2 + high * nb4, nb4)
    sq4 = send(sq_total.at[quarter], sq_total.at[quarter], sq_send.at[2], sq_recv.at[2], s, across)
    my_half = span(low * nb2, nb2)
    sq5 = send(sq_total.at[my_half], sq_total.at[my_half], sq_send.at[3], sq_recv.at[3], s, partner)

    def sq_row(j):
        row = lax.rem(s + j, row_count)
        return send(sq_rows.at[s], sq_rows.at[s], sq_row_send.at[j], sq_row_recv.at[s], row, g)

    def sq_row_from(j):
        source = lax.rem(s + j, row_count)
        return send(sq_rows.at[source], sq_rows.at[source], sq_row_send.at[j], sq_row_recv.at[source], source, g)

    positions = lax.broadcasted_iota(jnp.int32, (rows_dev, sample_count), 0)
    ones = jnp.ones((sample_count, width), BF16)

    def slot_tile(owner, slot):
        pair = pair_list[s, slot, owner]
        active = (slot < pair_count[s, owner]).astype(F32)
        first = pair_blocks[0, pair]
        second = pair_blocks[1, pair]
        picked = samples[first].reshape(1, sample_count)
        hits = jnp.where(positions == picked, 1.0, 0.0).astype(BF16)
        multiplicity = jnp.dot(hits, ones, preferred_element_type=F32)
        left = mat[first].astype(F32)
        right = mat[second]
        weighted = (multiplicity * active * left).astype(BF16)
        return lax.dot_general(
            weighted, right, (((0,), (0,)), ((), ())), preferred_element_type=F32
        )

    def core_copy(j):
        return send(core_out.at[j], core_in.at[j], core_send.at[j], core_recv.at[j], s, partner)

    top = lax.div(s, row_half)

    def far(j):
        return (1 - top) * row_half + lax.rem(s + j, row_half)

    def near(j):
        return top * row_half + lax.rem(s + j, row_half)

    mine = pl.ds(high * quota, quota)
    theirs = pl.ds((1 - high) * quota, quota)

    def high_copy(j):
        return send(keep.at[j, theirs], high_in.at[j], high_send.at[j], high_recv.at[j], s, across)

    def far_copy(j):
        return send(keep.at[j, mine], row_in.at[s, mine], row_send.at[j], row_recv.at[s], far(j), g)

    def far_from(j):
        source = far(j)
        return send(keep.at[j, mine], row_in.at[source, mine], row_send.at[j], row_recv.at[source], source, g)

    whole = pl.ds(0, half)

    def near_copy(j):
        k = row_half + j
        return send(keep.at[k], row_in.at[s, whole], row_send.at[k], row_recv.at[s], near(j), g)

    def near_from(j):
        k = row_half + j
        source = near(j)
        return send(keep.at[k], row_in.at[source, whole], row_send.at[k], row_recv.at[source], source, g)

    def make(j, owner):
        for n in range(half):
            core_out[j, n] = slot_tile(owner, (1 - low) * half + n)
        core_copy(j).start()
        for n in range(half):
            keep[j, n] = slot_tile(owner, low * half + n)

    def fold(j):
        core_copy(j).wait_recv()
        keep[j] = keep[j] + core_in[j]

    def fold_far(j):
        fold(j)
        high_copy(j).start()

    def cross(j):
        high_copy(j).wait_recv()
        keep[j, mine] = keep[j, mine] + high_in[j]
        far_copy(j).start()

    def fold_near(j):
        fold(row_half + j)
        near_copy(j).start()

    sq1.start()
    make(0, far(0))
    sq1.wait()
    sq_half[...] = squares[my_half, :] + sq_in[...]
    sq2.start()
    make(1, far(1))
    fold_far(0)

    def far_step(j, carry):
        make(j, far(j))
        fold_far(j - 1)
        cross(j - 2)
        return carry

    lax.fori_loop(2, row_half, far_step, 0)
    sq2.wait()
    sq_rows[s] = sq_half[span(high * nb4, nb4), :] + sq_in2[...]

    def sq_go(j, carry):
        sq_row(j).start()
        return carry

    lax.fori_loop(1, row_count, sq_go, 0)
    fold_far(row_half - 1)
    make(row_half + 1, near(1))
    cross(row_half - 2)
    make(row_half + 2, near(2))
    fold_near(1)
    cross(row_half - 1)

    def near_step(j, carry):
        make(row_half + j, near(j))
        fold_near(j - 1)
        return carry

    lax.fori_loop(3, row_half, near_step, 0)
    make(row_half, s)
    fold_near(row_half - 1)
    core_copy(row_half).wait_recv()
    row_in[s, whole] = keep[row_half] + core_in[row_half]

    def sq_done(j, carry):
        sq_row_from(j).wait_recv()
        return carry

    lax.fori_loop(1, row_count, sq_done, 0)
    sq_sum = sq_rows[0]
    for j in range(1, row_count):
        sq_sum = sq_sum + sq_rows[j]
    sq_total[quarter, :] = sq_sum
    sq4.start()

    def near_done(j, carry):
        near_from(j).wait_recv()
        return carry

    def far_done(j, carry):
        far_from(j).wait_recv()
        return carry

    lax.fori_loop(1, row_half, near_done, 0)
    lax.fori_loop(0, row_half, far_done, 0)

    def owned(grp, n):
        pair = s * region + grp * tile_dev + n
        total = None
        for j in range(row_count):
            source = far(j) if j < row_half else near(j - row_half)
            index = half
            for m in range(quota if j < row_half else half):
                place = m + high * quota if j < row_half else m
                same = (pair_list[source, low * half + place, s] == pair).astype(jnp.int32)
                index = jnp.minimum(index, half - (half - place) * same)
            tile = row_in[source, index]
            total = tile if total is None else total + tile
        return total

    def a_copy(n):
        return send(part_a.at[n], in_a.at[n], a_send.at[n], a_recv.at[n], s, partner)

    def b_copy(n):
        return send(part_b.at[n], in_b.at[n], b_send.at[n], b_recv.at[n], s, across)

    c_copy = send(part_c, in_c, c_send, c_recv, s, partner)
    far_low = (1 - high) * 2 + low
    far_other = (1 - high) * 2 + (1 - low)

    def pass_on(n):
        a_copy(n).wait_recv()
        part_b[n] = part_b[n] + in_a[n]
        b_copy(n).start()

    def distant(n, carry):
        part_a[n] = owned(far_other, n)
        a_copy(n).start()
        part_b[n] = owned(far_low, n)

        @pl.when(n > 0)
        def _():
            pass_on(n - 1)

        return carry

    lax.fori_loop(0, tile_dev, distant, 0)
    pass_on(tile_dev - 1)
    sq4.wait()
    sq5.start()

    def near_other(n, carry):
        part_c[n] = owned(partner, n)
        return carry

    lax.fori_loop(0, tile_dev, near_other, 0)
    c_copy.start()

    def local(n, carry):
        part_d[n] = owned(g, n)
        return carry

    lax.fori_loop(0, tile_dev, local, 0)
    sq5.wait()
    c_copy.wait()
    sq_total[...] = jnp.sqrt(
        sq_total[...] / (rows_dev * row_count * grp_count) + epsilon
    )

    def finish(n, carry):
        pair = s * region + g * tile_dev + n
        first = pair_blocks[0, pair]
        second = pair_blocks[1, pair]
        left = jnp.broadcast_to(sq_total[first].reshape(1, width), (width, width)).T
        right = sq_total[second].reshape(1, width)
        b_copy(n).wait_recv()
        total = part_d[n] + in_c[n] + in_b[n]
        out[n] = total / (sample_count * left * right)
        return carry

    lax.fori_loop(0, tile_dev, finish, 0)

    def drain_tiles(n, carry):
        a_copy(n).wait_send()
        b_copy(n).wait_send()
        return carry

    lax.fori_loop(0, tile_dev, drain_tiles, 0)

    def drain_rows(j, carry):
        core_copy(j).wait_send()
        sq_row(j).wait_send()
        return carry

    def drain_far(j, carry):
        high_copy(j).wait_send()
        far_copy(j).wait_send()
        return carry

    def drain_near(j, carry):
        near_copy(j).wait_send()
        return carry

    lax.fori_loop(1, row_count, drain_rows, 0)
    core_copy(0).wait_send()
    lax.fori_loop(0, row_half, drain_far, 0)
    lax.fori_loop(1, row_half, drain_near, 0)


def shards(matrix, sample_rows, pair_list, pair_count, pair_blocks):
    rows_dev, column_count = matrix.shape
    block_count, sample_count = sample_rows.shape[1:]
    width = column_count // block_count
    row_count = lax.axis_size("rows")
    grp_count = lax.axis_size("grp")
    cap = pair_list.shape[2]
    pairs = pair_blocks.shape[0]
    tile_dev = pairs // (row_count * grp_count)
    half = cap // 2
    dma = pltpu.SemaphoreType.DMA

    def vmem(*shape):
        return pltpu.VMEM(shape, F32)

    some = vmem(tile_dev, width, width)
    nb2, nb4 = block_count // 2, block_count // 4
    return pl.pallas_call(
        functools.partial(kernel, (row_count, grp_count, cap, pairs)),
        out_shape=jax.ShapeDtypeStruct((tile_dev, width, width), F32),
        in_specs=[
            pl.BlockSpec(memory_space=pltpu.SMEM),
            pl.BlockSpec(memory_space=pltpu.SMEM),
            pl.BlockSpec(memory_space=pltpu.SMEM),
            pl.BlockSpec(memory_space=pl.ANY),
            pl.BlockSpec(memory_space=pl.ANY),
        ],
        out_specs=pl.BlockSpec(memory_space=pltpu.VMEM),
        scratch_shapes=[
            pltpu.VMEM((block_count, rows_dev, width), BF16),
            pltpu.VMEM((block_count, sample_count), jnp.int32),
            dma,
            vmem(block_count, width),
            vmem(nb2, width),
            vmem(nb2, width),
            vmem(nb4, width),
            vmem(row_count, nb4, width),
            vmem(block_count, width),
            vmem(row_count, half, width, width),
            vmem(row_count, half, width, width),
            vmem(row_count, half, width, width),
            vmem(row_count // 2, half // 2, width, width),
            vmem(row_count, half + 1, width, width),
            some, some, some, some, some, some, some,
            dma((block_count,)), dma((4,)), dma((4,)), dma((row_count,)), dma((row_count,)),
            dma((row_count,)), dma((row_count,)), dma((row_count // 2,)), dma((row_count // 2,)),
            dma((row_count,)), dma((row_count,)),
            dma((tile_dev,)), dma((tile_dev,)), dma((tile_dev,)), dma((tile_dev,)),
            dma, dma,
        ],
        compiler_params=pltpu.CompilerParams(
            collective_id=0, has_side_effects=True, vmem_limit_bytes=67043328
        ),
        name="gram_tiles",
    )(pair_list.transpose(0, 2, 1), pair_count, pair_blocks.T, sample_rows[0], matrix)


def solution(mesh):
    in_specs = (P(("rows", "grp"), None), P(("rows", "grp"), None, None), P(), P(), P())
    out_specs = P(("rows", "grp"), None, None)
    return jax.shard_map(shards, mesh=mesh, in_specs=in_specs, out_specs=out_specs, check_vma=False)
```

```python
import functools

import jax
import jax.numpy as jnp
from jax import lax
from jax.experimental import pallas as pl
from jax.experimental.pallas import tpu as pltpu
from jax.sharding import PartitionSpec as P

epsilon = 1e-06
MESH = pl.DeviceIdType.MESH
F32 = jnp.float32
BF16 = jnp.bfloat16


def kernel(
    dims, pair_list, pair_count, pair_blocks, samples_hbm, matrix, out,
    mat, samples, sample_sem, squares, sq_in, sq_half, sq_in2, sq_rows, sq_total,
    core_out, core_in, keep, high_in, row_in0, row_in1, part_a, part_b, part_c, part_d, in_a, in_b, in_c,
    load_sem, sq_send, sq_recv, sq_row_send, sq_row_recv,
    core_send, core_recv, high_send, high_recv, row_send, row_recv,
    a_send, a_recv, b_send, b_recv, c_send, c_recv,
):
    row_count, grp_count, cap, pairs = dims
    block_count, rows_dev, width = mat.shape
    sample_count = samples.shape[1]
    half = cap // 2
    region = pairs // row_count
    tile_dev = region // grp_count
    quota = half // 2
    row_half = row_count // 2

    s = lax.axis_index("rows")
    g = lax.axis_index("grp")
    low = lax.rem(g, 2)
    high = lax.div(g, 2)
    partner = high * 2 + (1 - low)
    across = (1 - high) * 2 + low

    def at(row, grp):
        return {"rows": row, "grp": grp}

    def send(source, target, send_sem, recv_sem, row, grp):
        return pltpu.make_async_remote_copy(
            src_ref=source, dst_ref=target, send_sem=send_sem, recv_sem=recv_sem,
            device_id=at(row, grp), device_id_type=MESH,
        )

    def load(i):
        source = matrix.at[:, pl.ds(pl.multiple_of(i * width, width), width)]
        return pltpu.make_async_copy(source, mat.at[i], load_sem.at[i])

    def load_go(i, carry):
        load(i).start()
        return carry

    sample_load = pltpu.make_async_copy(samples_hbm, samples, sample_sem)
    sample_load.start()
    lax.fori_loop(0, block_count, load_go, 0)

    barrier = pltpu.get_barrier_semaphore()
    pl.semaphore_signal(barrier, inc=1, device_id=at(s, partner), device_id_type=MESH)
    pl.semaphore_signal(barrier, inc=1, device_id=at(s, across), device_id_type=MESH)

    def greet(j, carry):
        row = lax.rem(s + j, row_count)
        pl.semaphore_signal(barrier, inc=1, device_id=at(row, g), device_id_type=MESH)
        return carry

    lax.fori_loop(1, row_count, greet, 0)

    row_in = (row_in0, row_in1)
    tall = width // 2
    lines_of = (pl.ds(0, tall), pl.ds(tall, tall))
    zero_tile = jnp.zeros((tall, width), F32)

    def clear(j, carry):
        for h in range(2):
            row_in[h][j, half] = zero_tile
        return carry

    lax.fori_loop(0, row_count, clear, 0)

    def square_group(n, carry):
        lines = []
        for m in range(8):
            load(n * 8 + m).wait()
        for m in range(8):
            values = mat[n * 8 + m].astype(F32)
            lines.append(jnp.sum(values * values, axis=0, keepdims=True))
        squares[pl.ds(pl.multiple_of(n * 8, 8), 8), :] = jnp.concatenate(lines, axis=0)
        return carry

    lax.fori_loop(0, block_count // 8, square_group, 0)
    sample_load.wait()
    pl.semaphore_wait(barrier, row_count + 1)

    nb2 = block_count // 2
    nb4 = block_count // 4

    def span(start, size):
        return pl.ds(pl.multiple_of(start, 8), size)

    sq1 = send(squares.at[span((1 - low) * nb2, nb2)], sq_in, sq_send.at[0], sq_recv.at[0], s, partner)
    sq2 = send(sq_half.at[span((1 - high) * nb4, nb4)], sq_in2, sq_send.at[1], sq_recv.at[1], s, across)
    quarter = span(low * nb2 + high * nb4, nb4)
    sq4 = send(sq_total.at[quarter], sq_total.at[quarter], sq_send.at[2], sq_recv.at[2], s, across)
    my_half = span(low * nb2, nb2)
    sq5 = send(sq_total.at[my_half], sq_total.at[my_half], sq_send.at[3], sq_recv.at[3], s, partner)

    def sq_row(j):
        row = lax.rem(s + j, row_count)
        return send(sq_rows.at[s], sq_rows.at[s], sq_row_send.at[j], sq_row_recv.at[s], row, g)

    def sq_row_from(j):
        source = lax.rem(s + j, row_count)
        return send(sq_rows.at[source], sq_rows.at[source], sq_row_send.at[j], sq_row_recv.at[source], source, g)

    positions = lax.broadcasted_iota(jnp.int32, (rows_dev, sample_count), 0)
    ones = jnp.ones((sample_count, width), BF16)

    def slot_tile(owner, slot):
        pair = pair_list[s, slot, owner]
        active = (slot < pair_count[s, owner]).astype(F32)
        first = pair_blocks[0, pair]
        second = pair_blocks[1, pair]
        picked = samples[first].reshape(1, sample_count)
        hits = jnp.where(positions == picked, 1.0, 0.0).astype(BF16)
        multiplicity = jnp.dot(hits, ones, preferred_element_type=F32)
        left = mat[first].astype(F32)
        right = mat[second]
        weighted = (multiplicity * active * left).astype(BF16)
        return lax.dot_general(
            weighted, right, (((0,), (0,)), ((), ())), preferred_element_type=F32
        )

    def core_copy(j):
        return send(core_out.at[j], core_in.at[j], core_send.at[j], core_recv.at[j], s, partner)

    top = lax.div(s, row_half)

    def far(j):
        return (1 - top) * row_half + lax.rem(s + j, row_half)

    def near(j):
        return top * row_half + lax.rem(s + j, row_half)

    mine = pl.ds(high * quota, quota)
    theirs = pl.ds((1 - high) * quota, quota)
    whole = pl.ds(0, half)
    last = row_count - 1

    def is_far(k):
        return (k == 0) | ((lax.rem(k, 2) == 1) & (k < last))

    def is_near(k):
        return (k > 0) & (lax.rem(k, 2) == 0)

    def far_at(j):
        return jnp.maximum(2 * j - 1, 0)

    def high_copy(k):
        return send(keep.at[k, theirs], high_in.at[k], high_send.at[k], high_recv.at[k], s, across)

    def far_copy(h, j):
        k = far_at(j)
        return send(
            keep.at[k, mine, lines_of[h]], row_in[h].at[s, mine],
            row_send.at[h * row_count + k], row_recv.at[h * row_count + s], far(j), g,
        )

    def far_from(h, j):
        k = far_at(j)
        source = far(j)
        return send(
            keep.at[k, mine, lines_of[h]], row_in[h].at[source, mine],
            row_send.at[h * row_count + k], row_recv.at[h * row_count + source], source, g,
        )

    def near_copy(h, j):
        k = 2 * j
        return send(
            keep.at[k, whole, lines_of[h]], row_in[h].at[s, whole],
            row_send.at[h * row_count + k], row_recv.at[h * row_count + s], near(j), g,
        )

    def near_from(h, j):
        k = 2 * j
        source = near(j)
        return send(
            keep.at[k, whole, lines_of[h]], row_in[h].at[source, whole],
            row_send.at[h * row_count + k], row_recv.at[h * row_count + source], source, g,
        )

    def owner_of(k):
        odd = lax.rem(k, 2)
        final = lax.div(k, last)
        other = jnp.maximum(odd, 1 - jnp.minimum(k, 1)) * (1 - final)
        j = lax.div(k + 1, 2) * (1 - final)
        return (top * (1 - other) + (1 - top) * other) * row_half + lax.rem(s + j, row_half)

    def make_out(k):
        owner = owner_of(k)
        for n in range(half):
            core_out[k, n] = slot_tile(owner, (1 - low) * half + n)
        core_copy(k).start()

    def make_keep(k):
        owner = owner_of(k)
        for n in range(half):
            keep[k, n] = slot_tile(owner, low * half + n)
        core_copy(k).wait_recv()
        keep[k] = keep[k] + core_in[k]

    def cross(k):
        high_copy(k).wait_recv()
        keep[k, mine] = keep[k, mine] + high_in[k]
        far_copy(0, lax.div(k + 1, 2)).start()

    sq1.start()
    fold_lag, cross_lag = 2, 5

    def step(i, carry):
        @pl.when(i < row_count)
        def _():
            make_out(i)

        @pl.when(i == 2)
        def _():
            sq1.wait()
            sq_half[...] = squares[my_half, :] + sq_in[...]
            sq2.start()

        k = i - fold_lag

        @pl.when((k >= 0) & (k < row_count))
        def _():
            make_keep(k)

            @pl.when(is_far(k))
            def _():
                high_copy(k).start()

            @pl.when(is_near(k))
            def _():
                near_copy(0, lax.div(k, 2)).start()

        @pl.when(i == 5)
        def _():
            sq2.wait()
            sq_rows[s] = sq_half[span(high * nb4, nb4), :] + sq_in2[...]

            def sq_go(j, carry):
                sq_row(j).start()
                return carry

            lax.fori_loop(1, row_count, sq_go, 0)

        m = i - cross_lag

        @pl.when((m >= 0) & (m < row_count))
        def _():
            @pl.when(is_far(m))
            def _():
                cross(m)

        return carry

    lax.fori_loop(0, row_count + cross_lag - 2, step, 0)

    def second_far(j, carry):
        far_copy(1, j).start()
        return carry

    def second_near(j, carry):
        near_copy(1, j).start()
        return carry

    lax.fori_loop(0, row_half, second_far, 0)
    lax.fori_loop(1, row_half, second_near, 0)
    for h in range(2):
        row_in[h][s, whole] = keep[last, whole, lines_of[h]]

    def sq_done(j, carry):
        sq_row_from(j).wait_recv()
        return carry

    lax.fori_loop(1, row_count, sq_done, 0)
    sq_sum = sq_rows[0]
    for j in range(1, row_count):
        sq_sum = sq_sum + sq_rows[j]
    sq_total[quarter, :] = sq_sum
    sq4.start()

    def arrive(h):
        def near_done(j, carry):
            near_from(h, j).wait_recv()
            return carry

        def far_done(j, carry):
            far_from(h, j).wait_recv()
            return carry

        lax.fori_loop(1, row_half, near_done, 0)
        lax.fori_loop(0, row_half, far_done, 0)

    def owned(h, grp, n):
        pair = s * region + grp * tile_dev + n
        total = None
        for j in range(row_count):
            source = far(j) if j < row_half else near(j - row_half)
            index = half
            for m in range(quota if j < row_half else half):
                place = m + high * quota if j < row_half else m
                same = (pair_list[source, low * half + place, s] == pair).astype(jnp.int32)
                index = jnp.minimum(index, half - (half - place) * same)
            tile = row_in[h][source, index]
            total = tile if total is None else total + tile
        return total

    def a_copy(h, n):
        k = h * tile_dev + n
        lines = lines_of[h]
        return send(part_a.at[n, lines], in_a.at[n, lines], a_send.at[k], a_recv.at[k], s, partner)

    def b_copy(h, n):
        k = h * tile_dev + n
        lines = lines_of[h]
        return send(part_b.at[n, lines], in_b.at[n, lines], b_send.at[k], b_recv.at[k], s, across)

    def c_copy(h):
        lines = lines_of[h]
        return send(part_c.at[:, lines], in_c.at[:, lines], c_send.at[h], c_recv.at[h], s, partner)

    far_low = (1 - high) * 2 + low
    far_other = (1 - high) * 2 + (1 - low)

    def combine(h):
        lines = lines_of[h]

        def pass_on(n):
            a_copy(h, n).wait_recv()
            part_b[n, lines] = part_b[n, lines] + in_a[n, lines]
            b_copy(h, n).start()

        def distant(n, carry):
            @pl.when(n < tile_dev)
            def _():
                part_a[n, lines] = owned(h, far_other, n)
                a_copy(h, n).start()
                part_b[n, lines] = owned(h, far_low, n)

            @pl.when(n >= 3)
            def _():
                pass_on(n - 3)

            return carry

        def near_other(n, carry):
            part_c[n, lines] = owned(h, partner, n)
            return carry

        def local(n, carry):
            part_d[n, lines] = owned(h, g, n)
            return carry

        lax.fori_loop(0, tile_dev + 3, distant, 0)
        lax.fori_loop(0, tile_dev, near_other, 0)
        c_copy(h).start()
        lax.fori_loop(0, tile_dev, local, 0)

    arrive(0)
    combine(0)
    sq4.wait()
    sq5.start()
    arrive(1)
    combine(1)
    sq5.wait()
    sq_total[...] = jnp.sqrt(
        sq_total[...] / (rows_dev * row_count * grp_count) + epsilon
    )
    for h in range(2):
        lines = lines_of[h]
        c_copy(h).wait()

        def finish(n, carry):
            pair = s * region + g * tile_dev + n
            first = pair_blocks[0, pair]
            second = pair_blocks[1, pair]
            left = jnp.broadcast_to(sq_total[first].reshape(1, width), (width, width)).T
            right = sq_total[second].reshape(1, width)
            b_copy(h, n).wait_recv()
            total = part_d[n, lines] + in_c[n, lines] + in_b[n, lines]
            scale = sample_count * left[h * tall : (h + 1) * tall] * right
            out[n, lines] = total / scale
            return carry

        lax.fori_loop(0, tile_dev, finish, 0)

        def drain_tiles(n, carry):
            a_copy(h, n).wait_send()
            b_copy(h, n).wait_send()
            return carry

        lax.fori_loop(0, tile_dev, drain_tiles, 0)

    def drain_rows(j, carry):
        core_copy(j).wait_send()
        sq_row(j).wait_send()
        return carry

    def drain_far(j, carry):
        high_copy(far_at(j)).wait_send()
        for h in range(2):
            far_copy(h, j).wait_send()
        return carry

    def drain_near(j, carry):
        for h in range(2):
            near_copy(h, j).wait_send()
        return carry

    lax.fori_loop(1, row_count, drain_rows, 0)
    core_copy(0).wait_send()
    lax.fori_loop(0, row_half, drain_far, 0)
    lax.fori_loop(1, row_half, drain_near, 0)


def shards(matrix, sample_rows, pair_list, pair_count, pair_blocks):
    rows_dev, column_count = matrix.shape
    block_count, sample_count = sample_rows.shape[1:]
    width = column_count // block_count
    row_count = lax.axis_size("rows")
    grp_count = lax.axis_size("grp")
    cap = pair_list.shape[2]
    pairs = pair_blocks.shape[0]
    tile_dev = pairs // (row_count * grp_count)
    half = cap // 2
    dma = pltpu.SemaphoreType.DMA

    def vmem(*shape):
        return pltpu.VMEM(shape, F32)

    some = vmem(tile_dev, width, width)
    nb2, nb4 = block_count // 2, block_count // 4
    return pl.pallas_call(
        functools.partial(kernel, (row_count, grp_count, cap, pairs)),
        out_shape=jax.ShapeDtypeStruct((tile_dev, width, width), F32),
        in_specs=[
            pl.BlockSpec(memory_space=pltpu.SMEM),
            pl.BlockSpec(memory_space=pltpu.SMEM),
            pl.BlockSpec(memory_space=pltpu.SMEM),
            pl.BlockSpec(memory_space=pl.ANY),
            pl.BlockSpec(memory_space=pl.ANY),
        ],
        out_specs=pl.BlockSpec(memory_space=pltpu.VMEM),
        scratch_shapes=[
            pltpu.VMEM((block_count, rows_dev, width), BF16),
            pltpu.VMEM((block_count, sample_count), jnp.int32),
            dma,
            vmem(block_count, width),
            vmem(nb2, width),
            vmem(nb2, width),
            vmem(nb4, width),
            vmem(row_count, nb4, width),
            vmem(block_count, width),
            vmem(row_count, half, width, width),
            vmem(row_count, half, width, width),
            vmem(row_count, half, width, width),
            vmem(row_count, half // 2, width, width),
            vmem(row_count, half + 1, width // 2, width),
            vmem(row_count, half + 1, width // 2, width),
            some, some, some, some, some, some, some,
            dma((block_count,)), dma((4,)), dma((4,)), dma((row_count,)), dma((row_count,)),
            dma((row_count,)), dma((row_count,)), dma((row_count,)), dma((row_count,)),
            dma((2 * row_count,)), dma((2 * row_count,)),
            dma((2 * tile_dev,)), dma((2 * tile_dev,)), dma((2 * tile_dev,)),
            dma((2 * tile_dev,)), dma((2,)), dma((2,)),
        ],
        compiler_params=pltpu.CompilerParams(
            collective_id=0, has_side_effects=True, vmem_limit_bytes=67043328
        ),
        name="gram_tiles",
    )(pair_list.transpose(0, 2, 1), pair_count, pair_blocks.T, sample_rows[0], matrix)


def solution(mesh):
    in_specs = (P(("rows", "grp"), None), P(("rows", "grp"), None, None), P(), P(), P())
    out_specs = P(("rows", "grp"), None, None)
    return jax.shard_map(shards, mesh=mesh, in_specs=in_specs, out_specs=out_specs, check_vma=False)
```

```python
import functools

import jax
import jax.numpy as jnp
from jax import lax
from jax.experimental import pallas as pl
from jax.experimental.pallas import tpu as pltpu
from jax.sharding import PartitionSpec as P

epsilon = 1e-06
MESH = pl.DeviceIdType.MESH
F32 = jnp.float32
BF16 = jnp.bfloat16


def kernel(
    dims, pair_list, pair_count, pair_blocks, samples_hbm, matrix, out,
    mat, samples, sample_sem, squares, sq_in, sq_half, sq_in2, sq_rows, sq_total,
    core_out, core_in, keep, high_in, row_in0, row_in1, part_a, part_b, part_c, part_d, in_a, in_b, in_c,
    load_sem, sq_send, sq_recv, sq_row_send, sq_row_recv,
    core_send, core_recv, high_send, high_recv, row_send, row_recv,
    a_send, a_recv, b_send, b_recv, c_send, c_recv,
):
    row_count, grp_count, cap, pairs = dims
    block_count, rows_dev, width = mat.shape
    sample_count = samples.shape[1]
    half = cap // 2
    region = pairs // row_count
    tile_dev = region // grp_count
    quota = half // 2
    row_half = row_count // 2

    s = lax.axis_index("rows")
    g = lax.axis_index("grp")
    low = lax.rem(g, 2)
    high = lax.div(g, 2)
    partner = high * 2 + (1 - low)
    across = (1 - high) * 2 + low

    def at(row, grp):
        return {"rows": row, "grp": grp}

    def send(source, target, send_sem, recv_sem, row, grp):
        return pltpu.make_async_remote_copy(
            src_ref=source, dst_ref=target, send_sem=send_sem, recv_sem=recv_sem,
            device_id=at(row, grp), device_id_type=MESH,
        )

    def load(i):
        source = matrix.at[:, pl.ds(pl.multiple_of(i * width, width), width)]
        return pltpu.make_async_copy(source, mat.at[i], load_sem.at[i])

    def load_go(i, carry):
        load(i).start()
        return carry

    sample_load = pltpu.make_async_copy(samples_hbm, samples, sample_sem)
    sample_load.start()
    lax.fori_loop(0, block_count, load_go, 0)

    barrier = pltpu.get_barrier_semaphore()
    pl.semaphore_signal(barrier, inc=1, device_id=at(s, partner), device_id_type=MESH)
    pl.semaphore_signal(barrier, inc=1, device_id=at(s, across), device_id_type=MESH)

    def greet(j, carry):
        row = lax.rem(s + j, row_count)
        pl.semaphore_signal(barrier, inc=1, device_id=at(row, g), device_id_type=MESH)
        return carry

    lax.fori_loop(1, row_count, greet, 0)

    row_in = (row_in0, row_in1)
    tall = width // 2
    lines_of = (pl.ds(0, tall), pl.ds(tall, tall))
    zero_tile = jnp.zeros((tall, width), F32)

    def clear(j, carry):
        for h in range(2):
            row_in[h][j, half] = zero_tile
        return carry

    lax.fori_loop(0, row_count, clear, 0)

    def square_group(n, carry):
        lines = []
        for m in range(8):
            load(n * 8 + m).wait()
        for m in range(8):
            values = mat[n * 8 + m].astype(F32)
            lines.append(jnp.sum(values * values, axis=0, keepdims=True))
        squares[pl.ds(pl.multiple_of(n * 8, 8), 8), :] = jnp.concatenate(lines, axis=0)
        return carry

    lax.fori_loop(0, block_count // 8, square_group, 0)
    sample_load.wait()
    pl.semaphore_wait(barrier, row_count + 1)

    nb2 = block_count // 2
    nb4 = block_count // 4

    def span(start, size):
        return pl.ds(pl.multiple_of(start, 8), size)

    sq1 = send(squares.at[span((1 - low) * nb2, nb2)], sq_in, sq_send.at[0], sq_recv.at[0], s, partner)
    sq2 = send(sq_half.at[span((1 - high) * nb4, nb4)], sq_in2, sq_send.at[1], sq_recv.at[1], s, across)
    quarter = span(low * nb2 + high * nb4, nb4)
    sq4 = send(sq_total.at[quarter], sq_total.at[quarter], sq_send.at[2], sq_recv.at[2], s, across)
    my_half = span(low * nb2, nb2)
    sq5 = send(sq_total.at[my_half], sq_total.at[my_half], sq_send.at[3], sq_recv.at[3], s, partner)

    def sq_row(j):
        row = lax.rem(s + j, row_count)
        return send(sq_rows.at[s], sq_rows.at[s], sq_row_send.at[j], sq_row_recv.at[s], row, g)

    def sq_row_from(j):
        source = lax.rem(s + j, row_count)
        return send(sq_rows.at[source], sq_rows.at[source], sq_row_send.at[j], sq_row_recv.at[source], source, g)

    positions = lax.broadcasted_iota(jnp.int32, (rows_dev, sample_count), 0)
    ones = jnp.ones((sample_count, width), BF16)

    def slot_tile(owner, slot):
        pair = pair_list[s, slot, owner]
        active = (slot < pair_count[s, owner]).astype(F32)
        first = pair_blocks[0, pair]
        second = pair_blocks[1, pair]
        picked = samples[first].reshape(1, sample_count)
        hits = jnp.where(positions == picked, 1.0, 0.0).astype(BF16)
        multiplicity = jnp.dot(hits, ones, preferred_element_type=F32)
        left = mat[first].astype(F32)
        right = mat[second]
        weighted = (multiplicity * active * left).astype(BF16)
        return lax.dot_general(
            weighted, right, (((0,), (0,)), ((), ())), preferred_element_type=F32
        )

    def core_copy(j):
        return send(core_out.at[j], core_in.at[j], core_send.at[j], core_recv.at[j], s, partner)

    top = lax.div(s, row_half)

    def far(j):
        return (1 - top) * row_half + lax.rem(s + j, row_half)

    def near(j):
        return top * row_half + lax.rem(s + j, row_half)

    mine = pl.ds(high * quota, quota)
    theirs = pl.ds((1 - high) * quota, quota)
    whole = pl.ds(0, half)
    last = row_count - 1

    def is_far(k):
        return k < row_half

    def is_near(k):
        return (k >= row_half) & (k < last)

    def high_copy(k):
        return send(keep.at[k, theirs], high_in.at[k], high_send.at[k], high_recv.at[k], s, across)

    def far_copy(h, j):
        k = j
        return send(
            keep.at[k, mine, lines_of[h]], row_in[h].at[s, mine],
            row_send.at[h * row_count + k], row_recv.at[h * row_count + s], far(j), g,
        )

    def far_from(h, j):
        k = j
        source = far(j)
        return send(
            keep.at[k, mine, lines_of[h]], row_in[h].at[source, mine],
            row_send.at[h * row_count + k], row_recv.at[h * row_count + source], source, g,
        )

    def near_copy(h, j):
        k = row_half + j - 1
        return send(
            keep.at[k, whole, lines_of[h]], row_in[h].at[s, whole],
            row_send.at[h * row_count + k], row_recv.at[h * row_count + s], near(j), g,
        )

    def near_from(h, j):
        k = row_half + j - 1
        source = near(j)
        return send(
            keep.at[k, whole, lines_of[h]], row_in[h].at[source, whole],
            row_send.at[h * row_count + k], row_recv.at[h * row_count + source], source, g,
        )

    def owner_of(k):
        other = 1 - lax.div(k, row_half)
        j = k + 1 - other
        return (top * (1 - other) + (1 - top) * other) * row_half + lax.rem(s + j, row_half)

    def make(k):
        owner = owner_of(k)
        sent = [slot_tile(owner, (1 - low) * half + n) for n in range(half)]
        kept = [slot_tile(owner, low * half + n) for n in range(half)]
        for n in range(half):
            core_out[k, n] = sent[n]
        core_copy(k).start()
        for n in range(half):
            keep[k, n] = kept[n]

    def fold(k):
        core_copy(k).wait_recv()
        keep[k] = keep[k] + core_in[k]

    def cross(k):
        high_copy(k).wait_recv()
        keep[k, mine] = keep[k, mine] + high_in[k]
        far_copy(0, k).start()

    sq1.start()
    fold_lag, cross_lag = 1, 3

    def step(i, carry):
        @pl.when(i < row_count)
        def _():
            make(i)

        @pl.when(i == 2)
        def _():
            sq1.wait()
            sq_half[...] = squares[my_half, :] + sq_in[...]
            sq2.start()

        k = i - fold_lag

        @pl.when((k >= 0) & (k < row_count))
        def _():
            fold(k)

            @pl.when(is_far(k))
            def _():
                high_copy(k).start()

            @pl.when(is_near(k))
            def _():
                near_copy(0, k - row_half + 1).start()

        @pl.when(i == 5)
        def _():
            sq2.wait()
            sq_rows[s] = sq_half[span(high * nb4, nb4), :] + sq_in2[...]

            def sq_go(j, carry):
                sq_row(j).start()
                return carry

            lax.fori_loop(1, row_count, sq_go, 0)

        m = i - cross_lag

        @pl.when((m >= 0) & (m < row_count))
        def _():
            @pl.when(is_far(m))
            def _():
                cross(m)

        return carry

    lax.fori_loop(0, row_count + fold_lag, step, 0)

    def second_far(j, carry):
        far_copy(1, j).start()
        return carry

    def second_near(j, carry):
        near_copy(1, j).start()
        return carry

    lax.fori_loop(0, row_half, second_far, 0)
    lax.fori_loop(1, row_half, second_near, 0)
    for h in range(2):
        row_in[h][s, whole] = keep[last, whole, lines_of[h]]

    def sq_done(j, carry):
        sq_row_from(j).wait_recv()
        return carry

    lax.fori_loop(1, row_count, sq_done, 0)
    sq_sum = sq_rows[0]
    for j in range(1, row_count):
        sq_sum = sq_sum + sq_rows[j]
    sq_total[quarter, :] = sq_sum
    sq4.start()

    def arrive(h):
        def near_done(j, carry):
            near_from(h, j).wait_recv()
            return carry

        def far_done(j, carry):
            far_from(h, j).wait_recv()
            return carry

        lax.fori_loop(1, row_half, near_done, 0)
        lax.fori_loop(0, row_half, far_done, 0)

    def owned(h, grp, n):
        pair = s * region + grp * tile_dev + n
        total = None
        for j in range(row_count):
            source = far(j) if j < row_half else near(j - row_half)
            index = half
            for m in range(quota if j < row_half else half):
                place = m + high * quota if j < row_half else m
                same = (pair_list[source, low * half + place, s] == pair).astype(jnp.int32)
                index = jnp.minimum(index, half - (half - place) * same)
            tile = row_in[h][source, index]
            total = tile if total is None else total + tile
        return total

    def a_copy(h, n):
        k = h * tile_dev + n
        lines = lines_of[h]
        return send(part_a.at[n, lines], in_a.at[n, lines], a_send.at[k], a_recv.at[k], s, partner)

    def b_copy(h, n):
        k = h * tile_dev + n
        lines = lines_of[h]
        return send(part_b.at[n, lines], in_b.at[n, lines], b_send.at[k], b_recv.at[k], s, across)

    def c_copy(h):
        lines = lines_of[h]
        return send(part_c.at[:, lines], in_c.at[:, lines], c_send.at[h], c_recv.at[h], s, partner)

    far_low = (1 - high) * 2 + low
    far_other = (1 - high) * 2 + (1 - low)

    def combine(h):
        lines = lines_of[h]

        def pass_on(n):
            a_copy(h, n).wait_recv()
            part_b[n, lines] = part_b[n, lines] + in_a[n, lines]
            b_copy(h, n).start()

        def distant(n, carry):
            @pl.when(n < tile_dev)
            def _():
                part_a[n, lines] = owned(h, far_other, n)
                a_copy(h, n).start()
                part_b[n, lines] = owned(h, far_low, n)

            @pl.when(n >= 3)
            def _():
                pass_on(n - 3)

            return carry

        def near_other(n, carry):
            part_c[n, lines] = owned(h, partner, n)
            return carry

        def local(n, carry):
            part_d[n, lines] = owned(h, g, n)
            return carry

        lax.fori_loop(0, tile_dev + 3, distant, 0)
        lax.fori_loop(0, tile_dev, near_other, 0)
        c_copy(h).start()
        lax.fori_loop(0, tile_dev, local, 0)

    arrive(0)
    combine(0)
    sq4.wait()
    sq5.start()
    arrive(1)
    combine(1)
    sq5.wait()
    sq_total[...] = jnp.sqrt(
        sq_total[...] / (rows_dev * row_count * grp_count) + epsilon
    )
    for h in range(2):
        lines = lines_of[h]
        c_copy(h).wait()

        def finish(n, carry):
            pair = s * region + g * tile_dev + n
            first = pair_blocks[0, pair]
            second = pair_blocks[1, pair]
            left = jnp.broadcast_to(sq_total[first].reshape(1, width), (width, width)).T
            right = sq_total[second].reshape(1, width)
            b_copy(h, n).wait_recv()
            total = part_d[n, lines] + in_c[n, lines] + in_b[n, lines]
            scale = sample_count * left[h * tall : (h + 1) * tall] * right
            out[n, lines] = total / scale
            return carry

        lax.fori_loop(0, tile_dev, finish, 0)

        def drain_tiles(n, carry):
            a_copy(h, n).wait_send()
            b_copy(h, n).wait_send()
            return carry

        lax.fori_loop(0, tile_dev, drain_tiles, 0)

    def drain_rows(j, carry):
        core_copy(j).wait_send()
        sq_row(j).wait_send()
        return carry

    def drain_far(j, carry):
        high_copy(j).wait_send()
        for h in range(2):
            far_copy(h, j).wait_send()
        return carry

    def drain_near(j, carry):
        for h in range(2):
            near_copy(h, j).wait_send()
        return carry

    lax.fori_loop(1, row_count, drain_rows, 0)
    core_copy(0).wait_send()
    lax.fori_loop(0, row_half, drain_far, 0)
    lax.fori_loop(1, row_half, drain_near, 0)


def shards(matrix, sample_rows, pair_list, pair_count, pair_blocks):
    rows_dev, column_count = matrix.shape
    block_count, sample_count = sample_rows.shape[1:]
    width = column_count // block_count
    row_count = lax.axis_size("rows")
    grp_count = lax.axis_size("grp")
    cap = pair_list.shape[2]
    pairs = pair_blocks.shape[0]
    tile_dev = pairs // (row_count * grp_count)
    half = cap // 2
    dma = pltpu.SemaphoreType.DMA

    def vmem(*shape):
        return pltpu.VMEM(shape, F32)

    some = vmem(tile_dev, width, width)
    nb2, nb4 = block_count // 2, block_count // 4
    return pl.pallas_call(
        functools.partial(kernel, (row_count, grp_count, cap, pairs)),
        out_shape=jax.ShapeDtypeStruct((tile_dev, width, width), F32),
        in_specs=[
            pl.BlockSpec(memory_space=pltpu.SMEM),
            pl.BlockSpec(memory_space=pltpu.SMEM),
            pl.BlockSpec(memory_space=pltpu.SMEM),
            pl.BlockSpec(memory_space=pl.ANY),
            pl.BlockSpec(memory_space=pl.ANY),
        ],
        out_specs=pl.BlockSpec(memory_space=pltpu.VMEM),
        scratch_shapes=[
            pltpu.VMEM((block_count, rows_dev, width), BF16),
            pltpu.VMEM((block_count, sample_count), jnp.int32),
            dma,
            vmem(block_count, width),
            vmem(nb2, width),
            vmem(nb2, width),
            vmem(nb4, width),
            vmem(row_count, nb4, width),
            vmem(block_count, width),
            vmem(row_count, half, width, width),
            vmem(row_count, half, width, width),
            vmem(row_count, half, width, width),
            vmem(row_count, half // 2, width, width),
            vmem(row_count, half + 1, width // 2, width),
            vmem(row_count, half + 1, width // 2, width),
            some, some, some, some, some, some, some,
            dma((block_count,)), dma((4,)), dma((4,)), dma((row_count,)), dma((row_count,)),
            dma((row_count,)), dma((row_count,)), dma((row_count,)), dma((row_count,)),
            dma((2 * row_count,)), dma((2 * row_count,)),
            dma((2 * tile_dev,)), dma((2 * tile_dev,)), dma((2 * tile_dev,)),
            dma((2 * tile_dev,)), dma((2,)), dma((2,)),
        ],
        compiler_params=pltpu.CompilerParams(
            collective_id=0, has_side_effects=True, vmem_limit_bytes=67043328
        ),
        name="gram_tiles",
    )(pair_list.transpose(0, 2, 1), pair_count, pair_blocks.T, sample_rows[0], matrix)


def solution(mesh):
    in_specs = (P(("rows", "grp"), None), P(("rows", "grp"), None, None), P(), P(), P())
    out_specs = P(("rows", "grp"), None, None)
    return jax.shard_map(shards, mesh=mesh, in_specs=in_specs, out_specs=out_specs, check_vma=False)
```

```python
import functools

import jax
import jax.numpy as jnp
from jax import lax
from jax.experimental import pallas as pl
from jax.experimental.pallas import tpu as pltpu
from jax.sharding import PartitionSpec as P

epsilon = 1e-06
MESH = pl.DeviceIdType.MESH
F32 = jnp.float32
BF16 = jnp.bfloat16


def kernel(
    dims, pair_list, pair_count, pair_blocks, samples_hbm, matrix, out,
    mat, samples, sample_sem, squares, sq_in, sq_half, sq_in2, sq_rows, sq_total,
    core_out, core_in, keep, high_in, row_in0, row_in1, part_a, part_b, part_c, part_d, in_a, in_b, in_c,
    load_sem, sq_send, sq_recv, sq_row_send, sq_row_recv,
    core_send, core_recv, high_send, high_recv, row_send, row_recv,
    a_send, a_recv, b_send, b_recv, c_send, c_recv,
):
    row_count, grp_count, cap, pairs = dims
    block_count, rows_dev, width = mat.shape
    sample_count = samples.shape[1]
    half = cap // 2
    region = pairs // row_count
    tile_dev = region // grp_count
    quota = half // 2
    row_half = row_count // 2

    s = lax.axis_index("rows")
    g = lax.axis_index("grp")
    low = lax.rem(g, 2)
    high = lax.div(g, 2)
    partner = high * 2 + (1 - low)
    across = (1 - high) * 2 + low

    def at(row, grp):
        return {"rows": row, "grp": grp}

    def send(source, target, send_sem, recv_sem, row, grp):
        return pltpu.make_async_remote_copy(
            src_ref=source, dst_ref=target, send_sem=send_sem, recv_sem=recv_sem,
            device_id=at(row, grp), device_id_type=MESH,
        )

    def load(i):
        source = matrix.at[:, pl.ds(pl.multiple_of(i * width, width), width)]
        return pltpu.make_async_copy(source, mat.at[i], load_sem.at[i])

    def load_go(i, carry):
        load(i).start()
        return carry

    sample_load = pltpu.make_async_copy(samples_hbm, samples, sample_sem)
    sample_load.start()
    lax.fori_loop(0, block_count, load_go, 0)

    barrier = pltpu.get_barrier_semaphore()
    pl.semaphore_signal(barrier, inc=1, device_id=at(s, partner), device_id_type=MESH)
    pl.semaphore_signal(barrier, inc=1, device_id=at(s, across), device_id_type=MESH)

    def greet(j, carry):
        row = lax.rem(s + j, row_count)
        pl.semaphore_signal(barrier, inc=1, device_id=at(row, g), device_id_type=MESH)
        return carry

    lax.fori_loop(1, row_count, greet, 0)

    row_in = (row_in0, row_in1)
    tall = width // 2
    lines_of = (pl.ds(0, tall), pl.ds(tall, tall))
    zero_tile = jnp.zeros((tall, width), F32)

    def clear(j, carry):
        for h in range(2):
            row_in[h][j, half] = zero_tile
        return carry

    lax.fori_loop(0, row_count, clear, 0)

    def square_group(n, carry):
        lines = []
        for m in range(8):
            load(n * 8 + m).wait()
        for m in range(8):
            values = mat[n * 8 + m].astype(F32)
            lines.append(jnp.sum(values * values, axis=0, keepdims=True))
        squares[pl.ds(pl.multiple_of(n * 8, 8), 8), :] = jnp.concatenate(lines, axis=0)
        return carry

    lax.fori_loop(0, block_count // 8, square_group, 0)
    sample_load.wait()
    pl.semaphore_wait(barrier, row_count + 1)

    nb2 = block_count // 2
    nb4 = block_count // 4

    def span(start, size):
        return pl.ds(pl.multiple_of(start, 8), size)

    sq1 = send(squares.at[span((1 - low) * nb2, nb2)], sq_in, sq_send.at[0], sq_recv.at[0], s, partner)
    sq2 = send(sq_half.at[span((1 - high) * nb4, nb4)], sq_in2, sq_send.at[1], sq_recv.at[1], s, across)
    quarter = span(low * nb2 + high * nb4, nb4)
    sq4 = send(sq_total.at[quarter], sq_total.at[quarter], sq_send.at[2], sq_recv.at[2], s, across)
    my_half = span(low * nb2, nb2)
    sq5 = send(sq_total.at[my_half], sq_total.at[my_half], sq_send.at[3], sq_recv.at[3], s, partner)

    def sq_row(j):
        row = lax.rem(s + j, row_count)
        return send(sq_rows.at[s], sq_rows.at[s], sq_row_send.at[j], sq_row_recv.at[s], row, g)

    def sq_row_from(j):
        source = lax.rem(s + j, row_count)
        return send(sq_rows.at[source], sq_rows.at[source], sq_row_send.at[j], sq_row_recv.at[source], source, g)

    positions = lax.broadcasted_iota(jnp.int32, (rows_dev, sample_count), 0)
    ones = jnp.ones((sample_count, width), BF16)

    def slot_tile(owner, slot):
        pair = pair_list[s, slot, owner]
        active = (slot < pair_count[s, owner]).astype(F32)
        first = pair_blocks[0, pair]
        second = pair_blocks[1, pair]
        picked = samples[first].reshape(1, sample_count)
        hits = jnp.where(positions == picked, 1.0, 0.0).astype(BF16)
        multiplicity = jnp.dot(hits, ones, preferred_element_type=F32)
        left = mat[first].astype(F32)
        right = mat[second]
        weighted = (multiplicity * active * left).astype(BF16)
        return lax.dot_general(
            weighted, right, (((0,), (0,)), ((), ())), preferred_element_type=F32
        )

    def core_copy(j):
        return send(core_out.at[j], core_in.at[j], core_send.at[j], core_recv.at[j], s, partner)

    top = lax.div(s, row_half)

    def far(j):
        return (1 - top) * row_half + lax.rem(s + j, row_half)

    def near(j):
        return top * row_half + lax.rem(s + j, row_half)

    mine = pl.ds(high * quota, quota)
    theirs = pl.ds((1 - high) * quota, quota)
    whole = pl.ds(0, half)
    last = row_count - 1

    def is_far(k):
        return k < row_half

    def is_near(k):
        return (k >= row_half) & (k < last)

    def high_copy(k):
        return send(keep.at[k, theirs], high_in.at[k], high_send.at[k], high_recv.at[k], s, across)

    def far_copy(h, j):
        k = j
        return send(
            keep.at[k, mine, lines_of[h]], row_in[h].at[s, mine],
            row_send.at[h * row_count + k], row_recv.at[h * row_count + s], far(j), g,
        )

    def far_from(h, j):
        k = j
        source = far(j)
        return send(
            keep.at[k, mine, lines_of[h]], row_in[h].at[source, mine],
            row_send.at[h * row_count + k], row_recv.at[h * row_count + source], source, g,
        )

    def near_copy(h, j):
        k = row_half + j - 1
        return send(
            keep.at[k, whole, lines_of[h]], row_in[h].at[s, whole],
            row_send.at[h * row_count + k], row_recv.at[h * row_count + s], near(j), g,
        )

    def near_from(h, j):
        k = row_half + j - 1
        source = near(j)
        return send(
            keep.at[k, whole, lines_of[h]], row_in[h].at[source, whole],
            row_send.at[h * row_count + k], row_recv.at[h * row_count + source], source, g,
        )

    def owner_of(k):
        other = 1 - lax.div(k, row_half)
        j = k + 1 - other
        return (top * (1 - other) + (1 - top) * other) * row_half + lax.rem(s + j, row_half)

    def make(k):
        owner = owner_of(k)
        sent = [slot_tile(owner, (1 - low) * half + n) for n in range(half)]
        kept = [slot_tile(owner, low * half + n) for n in range(half)]
        for n in range(half):
            core_out[k, n] = sent[n]
        core_copy(k).start()
        for n in range(half):
            keep[k, n] = kept[n]

    def fold(k):
        core_copy(k).wait_recv()
        keep[k] = keep[k] + core_in[k]

    def cross(k):
        high_copy(k).wait_recv()
        keep[k, mine] = keep[k, mine] + high_in[k]
        far_copy(0, k).start()

    sq1.start()
    fold_lag, cross_lag = 1, 3

    def step(i, carry):
        @pl.when(i < row_count)
        def _():
            make(i)

        @pl.when(i == 1)
        def _():
            sq1.wait()
            sq_half[...] = squares[my_half, :] + sq_in[...]
            sq2.start()

        k = i - fold_lag

        @pl.when((k >= 0) & (k < row_count))
        def _():
            fold(k)

            @pl.when(is_far(k))
            def _():
                high_copy(k).start()

            @pl.when(is_near(k))
            def _():
                near_copy(0, k - row_half + 1).start()

        @pl.when(i == 4)
        def _():
            sq2.wait()
            sq_rows[s] = sq_half[span(high * nb4, nb4), :] + sq_in2[...]

            def sq_go(j, carry):
                sq_row(j).start()
                return carry

            lax.fori_loop(1, row_count, sq_go, 0)

        m = i - cross_lag

        @pl.when((m >= 0) & (m < row_count))
        def _():
            @pl.when(is_far(m))
            def _():
                cross(m)

        return carry

    lax.fori_loop(0, row_count + fold_lag, step, 0)

    def second_far(j, carry):
        far_copy(1, j).start()
        return carry

    def second_near(j, carry):
        near_copy(1, j).start()
        return carry

    lax.fori_loop(0, row_half, second_far, 0)
    lax.fori_loop(1, row_half, second_near, 0)
    for h in range(2):
        row_in[h][s, whole] = keep[last, whole, lines_of[h]]

    def sq_done(j, carry):
        sq_row_from(j).wait_recv()
        return carry

    lax.fori_loop(1, row_count, sq_done, 0)
    sq_sum = sq_rows[0]
    for j in range(1, row_count):
        sq_sum = sq_sum + sq_rows[j]
    sq_total[quarter, :] = sq_sum
    sq4.start()

    def arrive(h):
        def near_done(j, carry):
            near_from(h, j).wait_recv()
            return carry

        def far_done(j, carry):
            far_from(h, j).wait_recv()
            return carry

        lax.fori_loop(1, row_half, near_done, 0)
        lax.fori_loop(0, row_half, far_done, 0)

    def owned(h, grp, n):
        pair = s * region + grp * tile_dev + n
        total = None
        for j in range(row_count):
            source = far(j) if j < row_half else near(j - row_half)
            index = half
            for m in range(quota if j < row_half else half):
                place = m + high * quota if j < row_half else m
                same = (pair_list[source, low * half + place, s] == pair).astype(jnp.int32)
                index = jnp.minimum(index, half - (half - place) * same)
            tile = row_in[h][source, index]
            total = tile if total is None else total + tile
        return total

    def a_copy(h, n):
        k = h * tile_dev + n
        lines = lines_of[h]
        return send(part_a.at[n, lines], in_a.at[n, lines], a_send.at[k], a_recv.at[k], s, partner)

    def b_copy(h, n):
        k = h * tile_dev + n
        lines = lines_of[h]
        return send(part_b.at[n, lines], in_b.at[n, lines], b_send.at[k], b_recv.at[k], s, across)

    def c_copy(h):
        lines = lines_of[h]
        return send(part_c.at[:, lines], in_c.at[:, lines], c_send.at[h], c_recv.at[h], s, partner)

    far_low = (1 - high) * 2 + low
    far_other = (1 - high) * 2 + (1 - low)

    def combine(h):
        lines = lines_of[h]

        def pass_on(n):
            a_copy(h, n).wait_recv()
            part_b[n, lines] = part_b[n, lines] + in_a[n, lines]
            b_copy(h, n).start()

        def distant(n, carry):
            @pl.when(n < tile_dev)
            def _():
                part_a[n, lines] = owned(h, far_other, n)
                a_copy(h, n).start()
                part_b[n, lines] = owned(h, far_low, n)

            @pl.when(n >= 3)
            def _():
                pass_on(n - 3)

            return carry

        def near_other(n, carry):
            part_c[n, lines] = owned(h, partner, n)
            return carry

        def local(n, carry):
            part_d[n, lines] = owned(h, g, n)
            return carry

        lax.fori_loop(0, tile_dev + 3, distant, 0)
        lax.fori_loop(0, tile_dev, near_other, 0)
        c_copy(h).start()
        lax.fori_loop(0, tile_dev, local, 0)

    arrive(0)
    combine(0)
    sq4.wait()
    sq5.start()
    arrive(1)
    combine(1)
    sq5.wait()
    sq_total[...] = jnp.sqrt(
        sq_total[...] / (rows_dev * row_count * grp_count) + epsilon
    )
    for h in range(2):
        lines = lines_of[h]
        c_copy(h).wait()

        def finish(n, carry):
            pair = s * region + g * tile_dev + n
            first = pair_blocks[0, pair]
            second = pair_blocks[1, pair]
            left = jnp.broadcast_to(sq_total[first].reshape(1, width), (width, width)).T
            right = sq_total[second].reshape(1, width)
            b_copy(h, n).wait_recv()
            total = part_d[n, lines] + in_c[n, lines] + in_b[n, lines]
            scale = sample_count * left[h * tall : (h + 1) * tall] * right
            out[n, lines] = total / scale
            return carry

        lax.fori_loop(0, tile_dev, finish, 0)

        def drain_tiles(n, carry):
            a_copy(h, n).wait_send()
            b_copy(h, n).wait_send()
            return carry

        lax.fori_loop(0, tile_dev, drain_tiles, 0)

    def drain_rows(j, carry):
        core_copy(j).wait_send()
        sq_row(j).wait_send()
        return carry

    def drain_far(j, carry):
        high_copy(j).wait_send()
        for h in range(2):
            far_copy(h, j).wait_send()
        return carry

    def drain_near(j, carry):
        for h in range(2):
            near_copy(h, j).wait_send()
        return carry

    lax.fori_loop(1, row_count, drain_rows, 0)
    core_copy(0).wait_send()
    lax.fori_loop(0, row_half, drain_far, 0)
    lax.fori_loop(1, row_half, drain_near, 0)


def shards(matrix, sample_rows, pair_list, pair_count, pair_blocks):
    rows_dev, column_count = matrix.shape
    block_count, sample_count = sample_rows.shape[1:]
    width = column_count // block_count
    row_count = lax.axis_size("rows")
    grp_count = lax.axis_size("grp")
    cap = pair_list.shape[2]
    pairs = pair_blocks.shape[0]
    tile_dev = pairs // (row_count * grp_count)
    half = cap // 2
    dma = pltpu.SemaphoreType.DMA

    def vmem(*shape):
        return pltpu.VMEM(shape, F32)

    some = vmem(tile_dev, width, width)
    nb2, nb4 = block_count // 2, block_count // 4
    return pl.pallas_call(
        functools.partial(kernel, (row_count, grp_count, cap, pairs)),
        out_shape=jax.ShapeDtypeStruct((tile_dev, width, width), F32),
        in_specs=[
            pl.BlockSpec(memory_space=pltpu.SMEM),
            pl.BlockSpec(memory_space=pltpu.SMEM),
            pl.BlockSpec(memory_space=pltpu.SMEM),
            pl.BlockSpec(memory_space=pl.ANY),
            pl.BlockSpec(memory_space=pl.ANY),
        ],
        out_specs=pl.BlockSpec(memory_space=pltpu.VMEM),
        scratch_shapes=[
            pltpu.VMEM((block_count, rows_dev, width), BF16),
            pltpu.VMEM((block_count, sample_count), jnp.int32),
            dma,
            vmem(block_count, width),
            vmem(nb2, width),
            vmem(nb2, width),
            vmem(nb4, width),
            vmem(row_count, nb4, width),
            vmem(block_count, width),
            vmem(row_count, half, width, width),
            vmem(row_count, half, width, width),
            vmem(row_count, half, width, width),
            vmem(row_count, half // 2, width, width),
            vmem(row_count, half + 1, width // 2, width),
            vmem(row_count, half + 1, width // 2, width),
            some, some, some, some, some, some, some,
            dma((block_count,)), dma((4,)), dma((4,)), dma((row_count,)), dma((row_count,)),
            dma((row_count,)), dma((row_count,)), dma((row_count,)), dma((row_count,)),
            dma((2 * row_count,)), dma((2 * row_count,)),
            dma((2 * tile_dev,)), dma((2 * tile_dev,)), dma((2 * tile_dev,)),
            dma((2 * tile_dev,)), dma((2,)), dma((2,)),
        ],
        compiler_params=pltpu.CompilerParams(
            collective_id=0, has_side_effects=True, vmem_limit_bytes=67043328
        ),
        name="gram_tiles",
    )(pair_list.transpose(0, 2, 1), pair_count, pair_blocks.T, sample_rows[0], matrix)


def solution(mesh):
    in_specs = (P(("rows", "grp"), None), P(("rows", "grp"), None, None), P(), P(), P())
    out_specs = P(("rows", "grp"), None, None)
    return jax.shard_map(shards, mesh=mesh, in_specs=in_specs, out_specs=out_specs, check_vma=False)
```
